32 devices in a mesh: dp: 8 (over z, y), mp: 4 (over x, core).
Axes of the slice: x: 2, y: 2, z: 4, core: 2. Of those that a mesh axis runs over, the one named last changes fastest.
Arguments:
- gradients: bfloat16 [4, 16, 1024, 1024], P(None, 'mp', 'dp'), as said below
- statistics: float32 [4, 32, 1024, 1024], P('mp', 'dp'), as said below
- accumulator: float32 [4, 16, 1024, 1024], P(None, 'mp', 'dp'), may hold values from 0.25 to 4
Outputs:
- update: float32 [4, 16, 1024, 1024], P(None, 'mp', 'dp')
- statistics_new: float32 [4, 32, 1024, 1024], P('mp', 'dp')
- accumulator_new: float32 [4, 16, 1024, 1024], P(None, 'mp', 'dp')
The draws below stay inside these ranges and needn't reach their ends.
Inputs may be any that keep to these rules, and one draw needn't show every extreme that they name: `gradients`: Real-valued gradient blocks. `statistics`: each 1024 x 1024 statistic is symmetric positive definite.
All inputs are finite; a program needn't handle non-finite values.
Results may differ from the reference program's by a relative error of at most 0.005.
The reference program's roundings to bfloat16 on the way count: a program that leaves them out, or rounds other values in their place, can miss the bound.
Values may be sent and summed in bfloat16 or wider, within the bound.
A program may use at most 192 MiB of HBM per device.

```python
import math
import jax
import jax.numpy as jnp
from jax import lax

B = 1024
ITERS = 3
RB = 4
CB = 16
CB_MP = 4
BLKS = 16
N_MP = 4


def draw_gradients(key, part):
    subkeys = jax.random.split(key, 3)
    gaussian = jax.random.normal(subkeys[0], (RB, CB, B, B), jnp.float32)
    row_scale = 10.0 ** jax.random.uniform(subkeys[1], (RB, CB, B, 1), jnp.float32)
    col_scale = 10.0 ** jax.random.uniform(subkeys[2], (RB, CB, 1, B), jnp.float32)
    rising = (3.0 ** (jnp.arange(B, dtype=jnp.float32) / B))[:, None]
    values = gaussian * row_scale * col_scale * rising
    return values.astype(jnp.bfloat16)


def draw_statistics(key, part):
    spread = 2.0

    def one_matrix(position):
        matrix_key = jax.random.fold_in(key, position)
        noise_key, scale_key = jax.random.split(matrix_key)
        gaussian = jax.random.normal(noise_key, (B, B), jnp.float32)
        wishart = jnp.dot(gaussian, gaussian.T, precision=lax.Precision.HIGHEST) / B + 0.5 * jnp.eye(B, dtype=jnp.float32)
        diagonal_scale = jnp.exp(jax.random.uniform(scale_key, (B,), jnp.float32) * jnp.log(spread))
        return 0.25 * diagonal_scale[:, None] * wishart * diagonal_scale[None, :]
    matrices = lax.map(one_matrix, jnp.arange(N_MP * 2 * BLKS, dtype=jnp.int32))
    return matrices.reshape(N_MP, 2 * BLKS, B, B)


def shard_levels(own_key, extent, cuts, smallest, high):
    def one(dim, blocks):
        heights = jax.random.uniform(jax.random.fold_in(jax.random.fold_in(own_key, 6), dim), (blocks,), jnp.float32, smallest / len(cuts), high / len(cuts))
        return jnp.repeat(jnp.exp(heights), extent[dim] // blocks).reshape((-1,) + (1,) * (len(extent) - dim - 1))

    factor_of = one(*cuts[0])
    for cut in cuts[1:]:
        factor_of = factor_of * one(*cut)
    return factor_of


def setup_inputs(seed: int = 0) -> dict:
    streams_of = jax.random.split(jax.random.key(seed), 4)
    gradients = draw_gradients(jax.random.fold_in(streams_of[3], 71), 0)
    statistics = draw_statistics(jax.random.fold_in(streams_of[3], 71), 0)
    accumulator = jnp.clip(jnp.exp(math.log(4.0) - 2.7725887 * jax.random.uniform(streams_of[2], (RB, CB, B, B), jnp.float32) ** shard_levels(streams_of[2], (RB, CB, B, B), ((1, 4), (2, 8)), -0.2, 0.2)), 0.25, 4.0)
    return {"gradients": gradients, "statistics": statistics, "accumulator": accumulator}


def matmul(left, right):
    return jnp.dot(left.astype(jnp.float32), right.astype(jnp.float32), precision=lax.Precision.HIGHEST)

def inverse_root(statistic):
    identity = jnp.eye(statistic.shape[0], dtype=jnp.float32)
    frob_norm = jnp.sqrt(jnp.sum(statistic * statistic) + 1e-06)
    newton_scale = 2.5 / frob_norm
    matrix = newton_scale * statistic
    root_iter = jnp.sqrt(jnp.sqrt(newton_scale)) * identity
    for iteration in range(ITERS):
        factor = (1.25 * identity - 0.25 * matrix).astype(jnp.bfloat16)
        root_iter = matmul(root_iter.astype(jnp.bfloat16), factor)
        if iteration + 1 < ITERS:
            square = matmul(factor, factor).astype(jnp.bfloat16)
            fourth = matmul(square, square).astype(jnp.bfloat16)
            matrix = matmul(fourth, matrix.astype(jnp.bfloat16))
    return root_iter

def reference(gradients, statistics, accumulator):
    grads_wide = gradients.astype(jnp.float32)
    grad_total = jnp.sum(grads_wide * grads_wide)
    clip_factor = jnp.minimum(1.0, jnp.sqrt(RB * CB * B * B / (grad_total + 1e-06)))

    def one_block(position):
        mp_shard = position // BLKS
        local_block = position % BLKS
        row_block = (local_block // CB_MP).astype(jnp.int32)
        col_block = (mp_shard * CB_MP + local_block % CB_MP).astype(jnp.int32)
        zero_index = jnp.zeros((), jnp.int32)
        grad_block = lax.dynamic_slice(gradients, (row_block, col_block, zero_index, zero_index), (1, 1, B, B))[0, 0]
        stat_pair = lax.dynamic_slice(statistics, (mp_shard.astype(jnp.int32), (2 * local_block).astype(jnp.int32), zero_index, zero_index), (1, 2, B, B))[0]
        left_stat = 0.9 * stat_pair[0] + 0.1 / B * clip_factor * clip_factor * matmul(grad_block, grad_block.T)
        right_stat = 0.9 * stat_pair[1] + 0.1 / B * clip_factor * clip_factor * matmul(grad_block.T, grad_block)
        left_root = inverse_root(left_stat).astype(jnp.bfloat16)
        right_root = inverse_root(right_stat).astype(jnp.bfloat16)
        left_applied = matmul(left_root, grad_block).astype(jnp.bfloat16)
        product = matmul(left_applied, right_root)
        return (jnp.stack([left_stat, right_stat]), product)
    stats_all, products = lax.map(one_block, jnp.arange(N_MP * BLKS, dtype=jnp.int32))
    statistics_new = stats_all.reshape(N_MP, 2 * BLKS, B, B)
    preconditioned = products.reshape(N_MP, RB, CB_MP, B, B).transpose(1, 0, 2, 3, 4).reshape(RB, CB, B, B)
    scaled = clip_factor * grads_wide
    accumulated = accumulator + scaled * scaled
    graft_step = scaled / jnp.sqrt(accumulated)
    graft_ratio = jnp.sqrt(jnp.sum(graft_step * graft_step) / (jnp.sum(preconditioned * preconditioned) + 1e-06))
    return (graft_ratio * preconditioned, statistics_new, accumulated)
```

```python
import jax
import jax.numpy as jnp
from jax import lax
from jax.experimental import pallas as pl
from jax.experimental.pallas import tpu as pltpu
from jax.sharding import PartitionSpec as P

ITERS = 3


def partner_2(value, axis, distance):
    return lax.ppermute(value, axis, [(i, i ^ 1 << distance) for i in range(lax.axis_size(axis))])


def batch_dot(left, right):
    return jnp.einsum("kij,kjl->kil", left, right, preferred_element_type=jnp.float32)


def inverse_roots(statistic):
    block_width = statistic.shape[-1]
    identity = jnp.eye(block_width, dtype=jnp.float32)
    frob_norms = jnp.sqrt(jnp.sum(statistic * statistic, axis=(1, 2)) + 1e-06)
    newton_scale = (2.5 / frob_norms)[:, None, None]
    matrix = newton_scale * statistic
    root_iter = jnp.sqrt(jnp.sqrt(newton_scale)) * identity
    for iteration in range(ITERS):
        factor = (1.25 * identity - 0.25 * matrix).astype(jnp.bfloat16)
        root_iter = batch_dot(root_iter.astype(jnp.bfloat16), factor)
        if iteration + 1 < ITERS:
            square = batch_dot(factor, factor).astype(jnp.bfloat16)
            fourth = batch_dot(square, square).astype(jnp.bfloat16)
            matrix = batch_dot(fourth, matrix.astype(jnp.bfloat16))
    return root_iter


def split_device(gradients, statistics, accumulator):
    owners = lax.axis_size("dp")
    own_index = lax.axis_index("dp")
    row_blocks, col_blocks, dev_rows, block_width = gradients.shape
    blocks = row_blocks * col_blocks
    owned_factors = statistics.shape[1]
    split_pairs = owned_factors == 1
    half_rows = dev_rows // 2
    parity = own_index % 2
    left_side = parity == 0
    by_block = gradients.reshape(blocks, dev_rows, block_width)
    grads_wide = gradients.astype(jnp.float32)
    grad_total = lax.psum(jnp.sum(grads_wide * grads_wide), ("dp", "mp"))
    entries = blocks * dev_rows * block_width * owners * lax.axis_size("mp")
    clip_factor = jnp.minimum(1.0, jnp.sqrt(entries / (grad_total + 1e-06)))
    scaled = clip_factor * grads_wide
    accumulated = accumulator + scaled * scaled
    graft_step = scaled / jnp.sqrt(accumulated)
    graft_squares = jnp.sum(graft_step * graft_step)
    row_parts = 2 if split_pairs else 1
    row_units = by_block.reshape(blocks * row_parts, dev_rows // row_parts, block_width)
    received = lax.all_to_all(row_units, "dp", split_axis=0, concat_axis=1, tiled=True)
    if split_pairs:
        partner_part = partner_2(received, "dp", 0)
        own_part = received.reshape(owners, 1, half_rows, block_width)
        partner_part = partner_part.reshape(owners, 1, half_rows, block_width)
        ordered = jnp.where(
            left_side,
            jnp.concatenate([own_part, partner_part], 1),
            jnp.concatenate([partner_part, own_part], 1),
        )
        whole_blocks = ordered.reshape(1, owners * dev_rows, block_width)
    else:
        whole_blocks = received
    transposed = jnp.swapaxes(whole_blocks, 1, 2)
    if split_pairs:
        factor_inputs = jnp.where(left_side, whole_blocks, transposed)
    else:
        factor_inputs = jnp.stack([whole_blocks, transposed], 1).reshape(
            owned_factors, block_width, block_width
        )
    gram_matrix = jnp.einsum(
        "kij,klj->kil", factor_inputs, factor_inputs, preferred_element_type=jnp.float32
    )
    statistics_new = (
        0.9 * statistics[0] + 0.1 / block_width * clip_factor * clip_factor * gram_matrix
    )
    root_values = inverse_roots(statistics_new).astype(jnp.bfloat16)
    if split_pairs:
        partner = partner_2(root_values, "dp", 0)
        left_root = jnp.where(left_side, root_values, partner)[0]
        right_root = jnp.where(left_side, partner, root_values)[0]
        left_rows = lax.dynamic_slice_in_dim(
            left_root.reshape(owners, 2, half_rows, block_width), parity, 1, 1
        )
        left_rows = left_rows.reshape(owners * half_rows, block_width)
        left_applied = jnp.dot(
            left_rows, whole_blocks[0], preferred_element_type=jnp.float32
        ).astype(jnp.bfloat16)
        product = jnp.dot(left_applied, right_root, preferred_element_type=jnp.float32)
        pieces = product.reshape(1, owners, half_rows, block_width)
    else:
        root_pairs = root_values.reshape(-1, 2, block_width, block_width)
        left_applied = batch_dot(root_pairs[:, 0], whole_blocks).astype(jnp.bfloat16)
        product = batch_dot(left_applied, root_pairs[:, 1])
        pieces = product.reshape(-1, owners, dev_rows, block_width)
    returned = lax.all_to_all(
        pieces.astype(jnp.bfloat16), "dp", split_axis=1, concat_axis=0, tiled=True
    ).astype(pieces.dtype)
    returned = returned.reshape(row_blocks, col_blocks, dev_rows, block_width)
    graft_total, update_total = lax.psum(
        (graft_squares, jnp.sum(returned * returned)), ("dp", "mp")
    )
    graft_ratio = jnp.sqrt(graft_total / (update_total + 1e-06))
    return (graft_ratio * returned, statistics_new[None], accumulated)


TILE = 512
CHUNK = 128


def refresh_kernel(slot, width, aliased, *refs):
    scale_ref, grad_hbm, stats_hbm = refs[:3]
    refs = refs[4:] if aliased else refs[3:]
    out_stats, product_ref, sum_ref = refs[:3]
    stat, pair, fr, sqr, fourth, mats, frob, in_sem, out_sem, grad_sem = refs[3:]
    tile = min(TILE, width)
    tiles = width // tile
    dot = lambda a, b: jnp.dot(a, b, preferred_element_type=jnp.float32)

    grad_copy = pltpu.make_async_copy(grad_hbm, pair.at[0], grad_sem)
    grad_copy.start()
    loads = [
        pltpu.make_async_copy(stats_hbm.at[2 * slot + s], stat.at[s], in_sem.at[s])
        for s in range(2)
    ]
    for load in loads:
        load.start()
    grad_copy.wait()

    @pl.loop(0, width // CHUNK)
    def _(i):
        rows = pl.ds(pl.multiple_of(i * CHUNK, CHUNK), CHUNK)
        pair[1, :, rows] = pair[0, rows, :].T

    def over_tiles(count, body):
        @pl.loop(0, count * tiles)
        def _(i):
            body(i // tiles, pl.multiple_of(lax.rem(i, tiles) * tile, tile))

    def diagonal(row, rows):
        row_ids = lax.broadcasted_iota(jnp.int32, (rows, width), 0) + row
        return row_ids == lax.broadcasted_iota(jnp.int32, (rows, width), 1)

    scale = scale_ref[0]
    stores = [
        pltpu.make_async_copy(stat.at[s], out_stats.at[2 * slot + s], out_sem.at[s])
        for s in range(2)
    ]
    for s in range(2):
        loads[s].wait()
        frob[s] = jnp.zeros((8, width), jnp.float32)

        def gram(_, row, s=s):
            rows = pl.ds(row, tile)
            new = 0.9 * stat[s, rows, :] + scale * dot(pair[s, rows, :], pair[1 - s])
            stat[s, rows, :] = new
            frob[s] += jnp.sum((new * new).reshape(tile // 8, 8, width), axis=0)

        over_tiles(1, gram)
        stores[s].start()

    for s in range(2):
        total = jnp.sum(jnp.sum(frob[s], axis=0, keepdims=True), axis=1, keepdims=True)
        newton_scale = 2.5 / jnp.sqrt(total + 1e-06)
        first_root = jnp.sqrt(jnp.sqrt(newton_scale)).astype(jnp.bfloat16).astype(jnp.float32)

        @pl.loop(0, width // CHUNK)
        def _(i, s=s, newton_scale=newton_scale, first_root=first_root):
            row = pl.multiple_of(i * CHUNK, CHUNK)
            rows = pl.ds(row, CHUNK)
            matrix = newton_scale * stat[s, rows, :]
            quarter = -0.25 * matrix
            factor = jnp.where(diagonal(row, CHUNK), 1.25 + quarter, quarter)
            factor = factor.astype(jnp.bfloat16)
            fr[s, 0, rows, :] = factor
            fr[s, 1, rows, :] = (first_root * factor.astype(jnp.float32)).astype(jnp.bfloat16)
            mats[0, s, rows, :] = matrix.astype(jnp.bfloat16)

    def square(s, row):
        rows = pl.ds(row, tile)
        sqr[s, 0, rows, :] = dot(fr[s, 0, rows, :], fr[s, 0]).astype(jnp.bfloat16)

    def square_and_root(j, row):
        s, kind = j // 2, lax.rem(j, 2)
        rows = pl.ds(row, tile)
        sqr[s, kind, rows, :] = dot(fr[s, kind, rows, :], fr[s, 0]).astype(jnp.bfloat16)

    def power(s, row):
        rows = pl.ds(row, tile)
        fourth[s, rows, :] = dot(sqr[s, 0, rows, :], sqr[s, 0]).astype(jnp.bfloat16)

    def next_matrix(step):
        def body(s, row):
            rows = pl.ds(row, tile)
            matrix = dot(fourth[s, rows, :], mats[step, s])
            quarter = -0.25 * matrix
            factor = jnp.where(diagonal(row, tile), 1.25 + quarter, quarter)
            fr[s, 0, rows, :] = factor.astype(jnp.bfloat16)
            if step + 2 < ITERS:
                mats[step + 1, s, rows, :] = matrix.astype(jnp.bfloat16)

        return body

    over_tiles(2, square)
    for step in range(ITERS - 1):
        if step:
            over_tiles(4, square_and_root)
        over_tiles(2, power)
        over_tiles(2, next_matrix(step))

    def last_root(s, row):
        rows = pl.ds(row, tile)
        fr[s, 1, rows, :] = dot(sqr[s, 1, rows, :], fr[s, 0]).astype(jnp.bfloat16)

    over_tiles(2, last_root)

    def apply_left(_, row):
        rows = pl.ds(row, tile)
        pair[1, rows, :] = dot(fr[0, 1, rows, :], pair[0]).astype(jnp.bfloat16)

    over_tiles(1, apply_left)
    frob[0] = jnp.zeros((8, width), jnp.float32)

    def apply_right(_, row):
        rows = pl.ds(row, tile)
        product = dot(pair[1, rows, :], fr[1, 1])
        product_ref[rows, :] = product.astype(jnp.bfloat16)
        frob[0] += jnp.sum((product * product).reshape(tile // 8, 8, width), axis=0)

    over_tiles(1, apply_right)
    sum_ref[...] = frob[0]
    for store in stores:
        store.wait()


def refresh_block(slot, scale, block, statistics, previous):
    width = block.shape[-1]
    aliased = previous is not None
    hbm = pl.BlockSpec(memory_space=pl.ANY)
    vmem = pl.BlockSpec(memory_space=pltpu.VMEM)
    operands = (scale.reshape(1), block, statistics) + ((previous,) if aliased else ())
    return pl.pallas_call(
        lambda *refs: refresh_kernel(slot, width, aliased, *refs),
        out_shape=(
            jax.ShapeDtypeStruct(statistics.shape, jnp.float32),
            jax.ShapeDtypeStruct((width, width), jnp.bfloat16),
            jax.ShapeDtypeStruct((8, width), jnp.float32),
        ),
        in_specs=[pl.BlockSpec(memory_space=pltpu.SMEM)] + [hbm] * (len(operands) - 1),
        out_specs=(hbm, vmem, vmem),
        scratch_shapes=[
            pltpu.VMEM((2, width, width), jnp.float32),
            pltpu.VMEM((2, width, width), jnp.bfloat16),
            pltpu.VMEM((2, 2, width, width), jnp.bfloat16),
            pltpu.VMEM((2, 2, width, width), jnp.bfloat16),
            pltpu.VMEM((2, width, width), jnp.bfloat16),
            pltpu.VMEM((2, 2, width, width), jnp.bfloat16),
            pltpu.VMEM((2, 8, width), jnp.float32),
            pltpu.SemaphoreType.DMA((2,)),
            pltpu.SemaphoreType.DMA((2,)),
            pltpu.SemaphoreType.DMA,
        ],
        input_output_aliases={3: 0} if aliased else {},
        compiler_params=pltpu.CompilerParams(vmem_limit_bytes=56 * 2**20),
        cost_estimate=pl.CostEstimate(
            flops=40 * width**3, bytes_accessed=20 * width**2, transcendentals=0
        ),
        name=f"refresh_{slot}",
    )(*operands)


def finish_kernel(ratio_ref, *refs):
    out_ref = refs[-1]
    for slot, ref in enumerate(refs[:-1]):
        out_ref[0, slot] = ratio_ref[0] * ref[0].astype(jnp.float32)


def finish(ratio, returned):
    owners, dev_rows, width = returned[0].shape
    slots = len(returned)
    return pl.pallas_call(
        finish_kernel,
        grid=(owners,),
        out_shape=jax.ShapeDtypeStruct((owners, slots, dev_rows, width), jnp.float32),
        in_specs=[pl.BlockSpec(memory_space=pltpu.SMEM)]
        + [pl.BlockSpec((1, dev_rows, width), lambda i: (i, 0, 0))] * slots,
        out_specs=pl.BlockSpec((1, slots, dev_rows, width), lambda i: (i, 0, 0, 0)),
        name="finish",
    )(ratio.reshape(1), *returned)


def on_device(gradients, statistics, accumulator):
    owned_factors = statistics.shape[1]
    if owned_factors % 2:
        return split_device(gradients, statistics, accumulator)
    owners = lax.axis_size("dp")
    row_blocks, col_blocks, dev_rows, block_width = gradients.shape
    blocks = row_blocks * col_blocks
    slots = owned_factors // 2
    units = gradients.reshape(owners, slots, dev_rows, block_width)
    exchange = lambda rows: lax.all_to_all(rows, "dp", 0, 0, tiled=True)
    received = [exchange(units[:, 0])]
    grads_wide = gradients.astype(jnp.float32)
    grad_total = lax.psum(jnp.sum(grads_wide * grads_wide), ("dp", "mp"))
    entries = blocks * dev_rows * block_width * owners * lax.axis_size("mp")
    clip_factor = jnp.minimum(1.0, jnp.sqrt(entries / (grad_total + 1e-06)))
    scale = 0.1 / block_width * clip_factor * clip_factor
    for slot in range(1, slots):
        later, _ = lax.optimization_barrier((units[:, slot], scale))
        received.append(exchange(later))
    statistics_new = None
    returned = []
    update_squares = 0.0
    for slot in range(slots):
        whole_block = received[slot].reshape(block_width, block_width)
        statistics_new, product, squares = refresh_block(
            slot, scale, whole_block, statistics[0], statistics_new
        )
        update_squares = update_squares + jnp.sum(squares)
        returned.append(exchange(product.reshape(owners, dev_rows, block_width)))
    late_gradients, late_accumulator, update_squares = lax.optimization_barrier(
        (gradients, accumulator, update_squares)
    )
    scaled = clip_factor * late_gradients.astype(jnp.float32)
    accumulated = late_accumulator + scaled * scaled
    graft_step = scaled / jnp.sqrt(accumulated)
    graft_total, update_total = lax.psum(
        (jnp.sum(graft_step * graft_step), update_squares), ("dp", "mp")
    )
    graft_ratio = jnp.sqrt(graft_total / (update_total + 1e-06))
    update = finish(graft_ratio, returned).reshape(gradients.shape)
    return (update, statistics_new[None], accumulated)


def solution(mesh):
    return jax.shard_map(
        on_device,
        mesh=mesh,
        in_specs=(P(None, "mp", "dp", None), P("mp", "dp", None, None), P(None, "mp", "dp", None)),
        out_specs=(P(None, "mp", "dp", None), P("mp", "dp", None, None), P(None, "mp", "dp", None)),
        check_vma=False,
    )
```
